32 devices in a mesh: grp: 16 (over z, y, core), dev: 2 (over x).
Axes of the slice: x: 2, y: 2, z: 4, core: 2. Of those that a mesh axis runs over, the one named last changes fastest.
Arguments:
- stack: bfloat16 [608, 128, 512], P('grp', None, 'dev'), may hold values from -12 to 12
- network: int32 [608, 2], replicated, may hold values from 0 to 149, as said below
- bands: int32 [149], replicated, may hold values from 1 to 8
Outputs:
- deramped: bfloat16 [149, 128, 512], P(None, 'grp', 'dev')
- misfit: float32 [128, 512], P('grp', 'dev')
- spectrum: float32 [2, 149, 15, 15], replicated
The draws below stay inside these ranges and needn't reach their ends.
Inputs may be any that keep to these rules, and one draw needn't show every extreme that they name: `network`: each row holds a reference date and a later secondary date, both below 150; every pair of consecutive dates is some row.
All inputs are finite; a program needn't handle non-finite values.
Results may differ from the reference program's by a relative error of at most 0.005.
Values may be sent and summed in bfloat16 or wider, within the bound.
A program may use at most 128 MiB of HBM per device.

```python
import math
import jax
import jax.numpy as jnp
from jax import lax

DATES = 150
IFGS = 608
ROW_DEV = 8
BAND = 8
SOLVED = 149
FREQS = 15
ROWS = 128
COLS = 512


def draw_stack(key, part):
    first, second = jax.random.split(key, 2)
    noise = 1.5 * jax.random.truncated_normal(first, -4.0, 4.0, (IFGS, ROWS, COLS), jnp.float32)
    slopes = jax.random.uniform(second, (2, IFGS), jnp.float32, -6.0, 6.0)
    across = (jnp.arange(ROWS, dtype=jnp.float32) + 0.5) / ROWS - 0.5
    along = (jnp.arange(COLS, dtype=jnp.float32) + 0.5) / COLS - 0.5
    phase = noise + slopes[0][:, None, None] * across[None, :, None] + slopes[1][:, None, None] * along[None, None, :]
    return phase.astype(jnp.bfloat16)


def draw_network(key, part):
    first, second, third = jax.random.split(key, 3)
    extra = IFGS - (DATES - 1)
    chain_ref = jnp.arange(DATES - 1, dtype=jnp.int32)
    chain_sec = chain_ref + 1
    refs = jax.random.randint(first, (extra,), 0, DATES - 1, dtype=jnp.int32)
    gaps = jax.random.randint(second, (extra,), 0, DATES, dtype=jnp.int32)
    secs = refs + 1 + gaps % (DATES - 1 - refs)
    pairs = jnp.stack([jnp.concatenate([chain_ref, refs]), jnp.concatenate([chain_sec, secs])], axis=1)
    order = jax.random.permutation(third, IFGS)
    return pairs[order].astype(jnp.int32)


def set_ends(entries, stream_key, low, largest):
    extent = entries.shape
    index_at = [jax.random.randint(jax.random.fold_in(stream_key, axis), (), 0, extent[axis]) for axis in range(len(extent))]
    entries = entries.at[tuple(index_at)].set(low)
    longest = extent.index(max(extent))
    index_at[longest] = (index_at[longest] + 1) % extent[longest]
    return entries.at[tuple(index_at)].set(largest)


def setup_inputs(seed: int = 0) -> dict:
    splits = jax.random.split(jax.random.key(seed), 4)
    stack = draw_stack(jax.random.fold_in(splits[3], 71), 0)
    network = draw_network(jax.random.fold_in(splits[3], 71), 0)
    bands = set_ends(jax.random.randint(splits[2], (SOLVED,), 1, BAND + 1), jax.random.fold_in(splits[2], 1), 1, BAND).astype(jnp.int32)
    return {"stack": stack, "network": network, "bands": bands}


def build_inverse(network, solved):
    dates = jnp.arange(1, solved + 1, dtype=jnp.int32)
    design = (network[:, 1:2] == dates[None, :]).astype(jnp.float32) - (network[:, 0:1] == dates[None, :]).astype(jnp.float32)
    normal = jnp.dot(design.T, design, precision=lax.Precision.HIGHEST)
    factor = jnp.linalg.cholesky(normal)
    pinv = jax.scipy.linalg.cho_solve((factor, True), design.T)
    return (pinv.astype(jnp.bfloat16), design.astype(jnp.bfloat16))

def tables(positions, length, count):
    half = (count + 1) // 2
    steps = jnp.arange(count, dtype=jnp.int32) - (half - 1)
    turns = positions[:, None] * steps[None, :] % length
    angle = turns.astype(jnp.float32) * (2.0 * math.pi / length)
    return (jnp.cos(angle), jnp.sin(angle))

def reference(stack, network, bands):
    high = lax.Precision.HIGHEST
    pinv, design = build_inverse(network, SOLVED)
    blocks = ROWS // ROW_DEV

    def one_block(index):
        block = lax.dynamic_slice_in_dim(stack, (index * ROW_DEV).astype(jnp.int32), ROW_DEV, 1)
        flat = block.reshape(IFGS, ROW_DEV * COLS)
        series = jnp.dot(pinv.astype(jnp.float32), flat.astype(jnp.float32), preferred_element_type=jnp.float32)
        model = jnp.dot(design.astype(jnp.float32), series.astype(jnp.bfloat16).astype(jnp.float32), preferred_element_type=jnp.float32)
        resid = flat.astype(jnp.float32) - model
        misfit = jnp.sqrt(lax.optimization_barrier(jnp.mean(resid * resid, axis=0)) + 1e-06)
        return (series.reshape(SOLVED, ROW_DEV, COLS), misfit.reshape(ROW_DEV, COLS))
    series_blocks, misfit_blocks = lax.map(one_block, jnp.arange(blocks, dtype=jnp.int32))
    series = jnp.moveaxis(series_blocks, 0, 1).reshape(SOLVED, ROWS, COLS)
    misfit = misfit_blocks.reshape(ROWS, COLS)
    row_cos, row_sin = tables(jnp.arange(ROWS, dtype=jnp.int32), ROWS, FREQS)
    col_cos, col_sin = tables(jnp.arange(COLS, dtype=jnp.int32), COLS, FREQS)
    part_cos = jnp.einsum('thw,wl->thl', series, col_cos, precision=high)
    part_sin = jnp.einsum('thw,wl->thl', series, col_sin, precision=high)
    real = jnp.einsum('hk,thl->tkl', row_cos, part_cos, precision=high) - jnp.einsum('hk,thl->tkl', row_sin, part_sin, precision=high)
    imag = -(jnp.einsum('hk,thl->tkl', row_sin, part_cos, precision=high) + jnp.einsum('hk,thl->tkl', row_cos, part_sin, precision=high))
    scale = 1.0 / (ROWS * COLS)
    steps = jnp.abs(jnp.arange(FREQS, dtype=jnp.int32) - (BAND - 1))
    keep = (steps[None, :] < bands[:, None]).astype(jnp.float32)
    mask = keep[:, :, None] * keep[:, None, :]
    real = real * scale * mask
    imag = imag * scale * mask
    spectrum = jnp.stack([real, imag])
    rising = jnp.einsum('hk,tkl->thl', row_cos, real, precision=high) - jnp.einsum('hk,tkl->thl', row_sin, imag, precision=high)
    falling = -(jnp.einsum('hk,tkl->thl', row_sin, real, precision=high) + jnp.einsum('hk,tkl->thl', row_cos, imag, precision=high))
    ramp = jnp.einsum('thl,wl->thw', rising, col_cos, precision=high) + jnp.einsum('thl,wl->thw', falling, col_sin, precision=high)
    deramped = (series - ramp).astype(jnp.bfloat16)
    return (deramped, misfit, spectrum)
```

```python
import functools
import math

import jax
import jax.numpy as jnp
from jax import lax
from jax.experimental import pallas as pl
from jax.experimental.pallas import tpu as pltpu
from jax.sharding import PartitionSpec as P

BAND = 8
MESH = pl.DeviceIdType.MESH


def build_inverse(network, solved):
    dates = jnp.arange(1, solved + 1, dtype=jnp.int32)
    design = (network[:, 1:2] == dates[None, :]).astype(jnp.float32) - (
        network[:, 0:1] == dates[None, :]
    ).astype(jnp.float32)
    normal = jnp.dot(design.T, design, precision=lax.Precision.HIGHEST)
    factor = jnp.linalg.cholesky(normal)
    pinv = jax.scipy.linalg.cho_solve((factor, True), design.T)
    return (pinv.astype(jnp.bfloat16), design.astype(jnp.bfloat16))


def wave_tables(row_pos, rows_all, col_pos, cols_all):
    lanes = jnp.arange(2 * BAND * BAND, dtype=jnp.int32)
    row_step = lanes // BAND - (BAND - 1)
    col_step = lanes % BAND

    def waves(positions, steps, length):
        turns = positions[:, None] * steps[None, :] % length
        angle = turns.astype(jnp.float32) * (2.0 * math.pi / length)
        return jnp.concatenate([jnp.cos(angle), jnp.sin(angle)], axis=1)

    return waves(row_pos, row_step, rows_all), waves(col_pos, col_step, cols_all)


def basis(row, col):
    half = col.shape[1] // 2
    row_cos, row_sin = row[:, :half], row[:, half:]
    col_cos, col_sin = col[:, :half], col[:, half:]
    cos = row_cos * col_cos - row_sin * col_sin
    sin = row_sin * col_cos + row_cos * col_sin
    return jnp.concatenate([cos, sin], axis=1)


def split(x):
    high = x.astype(jnp.bfloat16)
    return high, (x - high.astype(jnp.float32)).astype(jnp.bfloat16)


def dot3(a, b, dims):
    a_hi, a_lo = split(a)
    b_hi, b_lo = split(b)
    dot = functools.partial(
        lax.dot_general,
        dimension_numbers=(dims, ((), ())),
        preferred_element_type=jnp.float32,
    )
    return dot(a_hi, b_hi) + (dot(a_hi, b_lo) + dot(a_lo, b_hi))


def invert_kernel(per, pinv, design, flat, row_wave, col_wave, series, fitted, parts, acc):
    h = pl.program_id(0)
    data = flat[...]
    out = jnp.dot(pinv[...], data, preferred_element_type=jnp.float32)
    series[...] = out
    model = jnp.dot(design[...], out.astype(jnp.bfloat16), preferred_element_type=jnp.float32)
    resid = data.astype(jnp.float32) - model
    mean = jnp.sum(resid * resid, axis=0, keepdims=True) * (1.0 / data.shape[0])
    fitted[pl.ds(h, 1), :] = jnp.sqrt(mean + 1e-06)
    part = dot3(out, basis(row_wave[pl.ds(h, 1), :], col_wave[...]), ((1,), (0,)))
    solved = part.shape[0]

    @pl.when(h == 0)
    def _():
        acc[...] = jnp.zeros_like(acc)

    acc[0:solved, :] += part

    @pl.when(h == pl.num_programs(0) - 1)
    def _():
        for j in range(parts.shape[0]):
            parts[j] = acc[j * per : (j + 1) * per, :]


def reduce_kernel(n_grp, n_dev, owners, x, y, got, send1, recv1, send2, recv2):
    count = n_grp * n_dev
    me = lax.axis_index("grp") * n_dev + lax.axis_index("dev")

    def coords(d):
        return (d // n_dev, d % n_dev)

    barrier = pltpu.get_barrier_semaphore()

    @pl.loop(1, count)
    def _(t):
        pl.semaphore_signal(
            barrier, inc=1, device_id=coords((me + t) % count), device_id_type=MESH
        )

    pl.semaphore_wait(barrier, count - 1)

    def scatter(dst):
        return pltpu.make_async_remote_copy(
            src_ref=x.at[dst],
            dst_ref=got.at[me],
            send_sem=send1.at[dst],
            recv_sem=recv1.at[me],
            device_id=coords(dst),
            device_id_type=MESH,
        )

    def gather(dst):
        return pltpu.make_async_remote_copy(
            src_ref=y.at[me],
            dst_ref=y.at[me],
            send_sem=send2.at[dst],
            recv_sem=recv2.at[me],
            device_id=coords(dst),
            device_id_type=MESH,
        )

    @pl.loop(1, count)
    def _(t):
        dst = (me + t) % count

        @pl.when(dst < owners)
        def _():
            scatter(dst).start()

    @pl.when(me < owners)
    def _():
        y[me] = x[me]

        @pl.loop(1, count)
        def _(t):
            src = (me + count - t) % count
            pltpu.make_async_remote_copy(
                src_ref=x.at[0],
                dst_ref=got.at[src],
                send_sem=send1.at[src],
                recv_sem=recv1.at[src],
                device_id=coords(src),
                device_id_type=MESH,
            ).wait_recv()
            y[me] += got[src]

        @pl.loop(1, count)
        def _(t):
            gather((me + t) % count).start()

    @pl.loop(1, count)
    def _(t):
        src = (me + count - t) % count

        @pl.when(src < owners)
        def _():
            pltpu.make_async_remote_copy(
                src_ref=y.at[0],
                dst_ref=y.at[src],
                send_sem=send2.at[src],
                recv_sem=recv2.at[src],
                device_id=coords(src),
                device_id_type=MESH,
            ).wait_recv()

    @pl.loop(1, count)
    def _(t):
        dst = (me + t) % count

        @pl.when(dst < owners)
        def _():
            scatter(dst).wait_send()

        @pl.when(me < owners)
        def _():
            gather(dst).wait_send()


def ramp_kernel(scale, coef, bands, series, row_wave, col_wave, deramped, masked, weighted):
    h = pl.program_id(0)

    @pl.when(h == 0)
    def _():
        lane = lax.broadcasted_iota(jnp.int32, coef.shape, 1) % (2 * BAND * BAND)
        row_step = jnp.abs(lane // BAND - (BAND - 1))
        col_step = lane % BAND
        keep = (row_step < bands[...]) & (col_step < bands[...])
        value = jnp.where(keep, coef[...] * scale, 0.0)
        masked[...] = value
        weighted[...] = jnp.where(col_step > 0, value + value, value)

    ramp = dot3(weighted[...], basis(row_wave[pl.ds(h, 1), :], col_wave[...]), ((1,), (1,)))
    deramped[...] = (series[...] - ramp).astype(jnp.bfloat16)


def on_device(stack, network, bands):
    solved = bands.shape[0]
    freqs = 2 * BAND - 1
    lanes = 4 * BAND * BAND
    pinv, design = build_inverse(network, solved)
    block = lax.all_to_all(stack, "grp", split_axis=1, concat_axis=0, tiled=True)
    ifgs, strip, items = block.shape
    flat = block.reshape(ifgs, strip * items)
    n_grp, n_dev = lax.axis_size("grp"), lax.axis_size("dev")
    count = n_grp * n_dev
    per = -(-solved // count)
    owners = -(-solved // per)
    rows_all, cols_all = strip * n_grp, items * n_dev
    row_pos = lax.axis_index("grp") * strip + jnp.arange(strip, dtype=jnp.int32)
    col_pos = lax.axis_index("dev") * items + jnp.arange(items, dtype=jnp.int32)
    row_wave, col_wave = wave_tables(row_pos, rows_all, col_pos, cols_all)

    whole = lambda *shape: pl.BlockSpec(shape, lambda h: (0,) * len(shape))
    tile = lambda rows: pl.BlockSpec((rows, items), lambda h: (0, h))
    series, fitted, parts = pl.pallas_call(
        functools.partial(invert_kernel, per),
        grid=(strip,),
        out_shape=(
            jax.ShapeDtypeStruct((solved, strip * items), jnp.float32),
            jax.ShapeDtypeStruct((strip, items), jnp.float32),
            jax.ShapeDtypeStruct((owners, per, lanes), jnp.float32),
        ),
        in_specs=[
            whole(solved, ifgs),
            whole(ifgs, solved),
            tile(ifgs),
            whole(strip, lanes),
            whole(items, lanes),
        ],
        out_specs=(tile(solved), whole(strip, items), whole(owners, per, lanes)),
        scratch_shapes=[pltpu.VMEM((owners * per, lanes), jnp.float32)],
        name="invert",
    )(pinv, design, flat, row_wave, col_wave)

    vmem = pl.BlockSpec(memory_space=pltpu.VMEM)
    coef = pl.pallas_call(
        functools.partial(reduce_kernel, n_grp, n_dev, owners),
        out_shape=jax.ShapeDtypeStruct((owners, per, lanes), jnp.float32),
        in_specs=[vmem],
        out_specs=vmem,
        scratch_shapes=[
            pltpu.VMEM((count, per, lanes), jnp.float32),
            pltpu.SemaphoreType.DMA((count,)),
            pltpu.SemaphoreType.DMA((count,)),
            pltpu.SemaphoreType.DMA((count,)),
            pltpu.SemaphoreType.DMA((count,)),
        ],
        compiler_params=pltpu.CompilerParams(collective_id=0, has_side_effects=True),
        name="exchange",
    )(parts)
    coef = coef.reshape(owners * per, lanes)[:solved]

    scale = 1.0 / (rows_all * cols_all)
    deramped, masked = pl.pallas_call(
        functools.partial(ramp_kernel, scale),
        grid=(strip,),
        out_shape=(
            jax.ShapeDtypeStruct((solved, strip * items), jnp.bfloat16),
            jax.ShapeDtypeStruct((solved, lanes), jnp.float32),
        ),
        in_specs=[
            whole(solved, lanes),
            whole(solved, 1),
            tile(solved),
            whole(strip, lanes),
            whole(items, lanes),
        ],
        out_specs=(tile(solved), whole(solved, lanes)),
        scratch_shapes=[pltpu.VMEM((solved, lanes), jnp.float32)],
        name="deramp",
    )(coef, bands[:, None], series, row_wave, col_wave)
    half = masked.reshape(solved, 2, 2 * BAND, BAND)[:, :, :freqs, :]
    mirror = half[:, :, ::-1, :0:-1]
    real = jnp.concatenate([mirror[:, 0], half[:, 0]], axis=2)
    imag = jnp.concatenate([mirror[:, 1], -half[:, 1]], axis=2)
    spectrum = jnp.stack([real, imag])
    return (deramped.reshape(solved, strip, items), fitted, spectrum)


def solution(mesh):
    return jax.shard_map(
        on_device,
        mesh=mesh,
        in_specs=(P("grp", None, "dev"), P(), P()),
        out_specs=(P(None, "grp", "dev"), P("grp", "dev"), P()),
        check_vma=False,
    )
```

```python
import functools
import math

import jax
import jax.numpy as jnp
import numpy as np
from jax import lax
from jax.experimental import pallas as pl
from jax.experimental.pallas import tpu as pltpu
from jax.sharding import PartitionSpec as P

BAND = 8
LANES = 128
MESH = pl.DeviceIdType.MESH


def wave_tables(row_pos, rows_all, col_pos, cols_all):
    lanes = jnp.arange(2 * BAND * BAND, dtype=jnp.int32)
    row_step = lanes // BAND - (BAND - 1)
    col_step = lanes % BAND

    def waves(positions, steps, length):
        turns = positions[:, None] * steps[None, :] % length
        angle = turns.astype(jnp.float32) * (2.0 * math.pi / length)
        return jnp.concatenate([jnp.cos(angle), jnp.sin(angle)], axis=1)

    return waves(row_pos, row_step, rows_all), waves(col_pos, col_step, cols_all)


def basis(row, col):
    half = col.shape[1] // 2
    row_cos, row_sin = row[:, :half], row[:, half:]
    col_cos, col_sin = col[:, :half], col[:, half:]
    cos = row_cos * col_cos - row_sin * col_sin
    sin = row_sin * col_cos + row_cos * col_sin
    return jnp.concatenate([cos, sin], axis=1)


def split(x):
    high = x.astype(jnp.bfloat16)
    return high, (x - high.astype(jnp.float32)).astype(jnp.bfloat16)


def dot3(a, b, dims):
    a_hi, a_lo = split(a)
    b_hi, b_lo = split(b)
    dot = functools.partial(
        lax.dot_general,
        dimension_numbers=(dims, ((), ())),
        preferred_element_type=jnp.float32,
    )
    return dot(a_hi, b_hi) + (dot(a_hi, b_lo) + dot(a_lo, b_hi))


def split3(x):
    high, rest = split(x)
    low, last = split(x - high.astype(jnp.float32))
    return high, low, last


def sweep(matrix, b):
    rows, lanes = matrix.shape
    lane = lax.broadcasted_iota(jnp.int32, (8, lanes), 1)
    sub = lax.broadcasted_iota(jnp.int32, (8, lanes), 0)
    panel = matrix[pl.ds(pl.multiple_of(b * 8, 8), 8), :]
    work = pltpu.roll(panel, lanes - b * 8, axis=1)
    for r in range(8):
        inv = 1.0 / work[r : r + 1, r : r + 1]
        row = jnp.where(lane[:1] == r, 1.0, work[r : r + 1, :]) * inv
        rest = jnp.where(lane == r, 0.0, work) - work[:, r : r + 1] * row
        work = jnp.where(sub == r, row, rest)
    work = pltpu.roll(work, b * 8, axis=1)
    inside = lane // 8 == b
    unit = jnp.where(lane == sub + b * 8, 1.0, 0.0)
    zero = jnp.where(inside, 0.0, work)
    left = jnp.concatenate([jnp.where(inside, 0.0, -panel), zero, unit], axis=0)
    right = jnp.concatenate([zero, unit, jnp.where(inside, -work, work)], axis=0)
    change = lax.dot_general(
        left[:, :rows],
        right,
        (((0,), (0,)), ((), ())),
        preferred_element_type=jnp.float32,
        precision=lax.Precision.HIGHEST,
    )
    row_of = lax.broadcasted_iota(jnp.int32, (rows, lanes), 0) // 8
    lane_of = lax.broadcasted_iota(jnp.int32, (rows, lanes), 1) // 8
    matrix[...] = jnp.where((row_of == b) | (lane_of == b), 0.0, matrix[...]) + change


def inverse(solved, network, design_t, matrix, pinv):
    rows, lanes = matrix.shape
    date = lax.broadcasted_iota(jnp.int32, design_t.shape, 0) + 1
    one = lambda k: jnp.where(network[k : k + 1, :] == date, 1.0, 0.0)
    design_t[...] = (one(1) - one(0)).astype(jnp.bfloat16)
    normal = lax.dot_general(
        design_t[...],
        design_t[...],
        (((1,), (1,)), ((), ())),
        preferred_element_type=jnp.float32,
    )[:rows]
    row = lax.broadcasted_iota(jnp.int32, (rows, lanes), 0)
    lane = lax.broadcasted_iota(jnp.int32, (rows, lanes), 1)
    matrix[...] = jnp.where((row == lane) & (row >= solved), 1.0, normal)

    @pl.loop(0, rows // 8)
    def _(b):
        sweep(matrix, b)

    total = None
    for piece in split3(-matrix[...]):
        term = jnp.dot(piece, design_t[...], preferred_element_type=jnp.float32)
        total = term if total is None else total + term
    pinv[...] = total.astype(jnp.bfloat16)


def kernel(
    n_grp, n_dev, solved, scale,
    stack, network, bands, row_wave, col_wave, choose,
    deramped, fitted, spectrum,
    block, data, design_t, matrix, pinv, series, acc, x, y, got, coef, flat,
    send0, recv0, own, send1, recv1, send2, recv2,
):
    count = n_grp * n_dev
    grp, dev = lax.axis_index("grp"), lax.axis_index("dev")
    me = grp * n_dev + dev
    ifgs, strip, items = block.shape
    share = stack.shape[0]
    owners, per, lanes = x.shape

    def coords(d):
        return (d // n_dev, d % n_dev)

    barrier = pltpu.get_barrier_semaphore()

    @pl.loop(1, count)
    def _(t):
        pl.semaphore_signal(
            barrier, inc=1, device_id=coords((me + t) % count), device_id_type=MESH
        )

    pl.semaphore_wait(barrier, count - 1)

    def trade(to, slot, place):
        return pltpu.make_async_remote_copy(
            src_ref=stack.at[:, pl.ds(pl.multiple_of(to * strip, strip), strip), :],
            dst_ref=block.at[pl.ds(place * share, share)],
            send_sem=send0.at[to],
            recv_sem=recv0.at[slot],
            device_id=(to, dev),
            device_id_type=MESH,
        )

    @pl.loop(1, n_grp)
    def _(t):
        trade((grp + t) % n_grp, grp, grp).start()

    local = pltpu.make_async_copy(
        stack.at[:, pl.ds(pl.multiple_of(grp * strip, strip), strip), :],
        block.at[pl.ds(grp * share, share)],
        own,
    )
    local.start()

    inverse(solved, network, design_t, matrix, pinv)

    def widen(src):
        piece = block[pl.ds(src * share, share)].astype(jnp.float32)
        start = pl.multiple_of(src * share * strip, strip)
        piece = piece.reshape(share * strip, items)
        for c in range(items // LANES):
            data[c, pl.ds(start, share * strip), :] = piece[:, c * LANES : (c + 1) * LANES]

    local.wait()
    widen(grp)

    @pl.loop(1, n_grp)
    def _(t):
        src = (grp + n_grp - t) % n_grp
        trade(src, src, src).wait_recv()
        widen(src)

    acc[...] = jnp.zeros_like(acc)

    @pl.loop(0, strip)
    def _(h):
        phase = jnp.concatenate(
            [data[c, pl.ds(h, ifgs, stride=strip), :] for c in range(items // LANES)], axis=1
        )
        out = jnp.dot(pinv[...], phase.astype(jnp.bfloat16), preferred_element_type=jnp.float32)
        series[h] = out
        model = lax.dot_general(
            design_t[0 : out.shape[0], :],
            out.astype(jnp.bfloat16),
            (((0,), (0,)), ((), ())),
            preferred_element_type=jnp.float32,
        )
        resid = phase - model
        mean = jnp.sum(resid * resid, axis=0, keepdims=True) * (1.0 / ifgs)
        fitted[pl.ds(h, 1), :] = jnp.sqrt(mean + 1e-06)
        acc[...] += dot3(out, basis(row_wave[pl.ds(h, 1), :], col_wave[...]), ((1,), (0,)))

    for j in range(owners):
        x[j] = acc[j * per : (j + 1) * per, :]

    def scatter(dst):
        return pltpu.make_async_remote_copy(
            src_ref=x.at[dst],
            dst_ref=got.at[me],
            send_sem=send1.at[dst],
            recv_sem=recv1.at[me],
            device_id=coords(dst),
            device_id_type=MESH,
        )

    def gather(dst):
        return pltpu.make_async_remote_copy(
            src_ref=y.at[me],
            dst_ref=y.at[me],
            send_sem=send2.at[dst],
            recv_sem=recv2.at[me],
            device_id=coords(dst),
            device_id_type=MESH,
        )

    @pl.loop(1, count)
    def _(t):
        dst = (me + t) % count

        @pl.when(dst < owners)
        def _():
            scatter(dst).start()

    @pl.when(me < owners)
    def _():
        y[me] = x[me]

        @pl.loop(1, count)
        def _(t):
            src = (me + count - t) % count
            pltpu.make_async_remote_copy(
                src_ref=x.at[0],
                dst_ref=got.at[src],
                send_sem=send1.at[src],
                recv_sem=recv1.at[src],
                device_id=coords(src),
                device_id_type=MESH,
            ).wait_recv()
            y[me] += got[src]

        @pl.loop(1, count)
        def _(t):
            gather((me + t) % count).start()

    @pl.loop(1, count)
    def _(t):
        src = (me + count - t) % count

        @pl.when(src < owners)
        def _():
            pltpu.make_async_remote_copy(
                src_ref=y.at[0],
                dst_ref=y.at[src],
                send_sem=send2.at[src],
                recv_sem=recv2.at[src],
                device_id=coords(src),
                device_id_type=MESH,
            ).wait_recv()

    coef[...] = jnp.zeros_like(coef)
    for j in range(owners):
        coef[j * per : (j + 1) * per, :] = y[j]

    lane = lax.broadcasted_iota(jnp.int32, coef.shape, 1) % (2 * BAND * BAND)
    row_step = jnp.abs(lane // BAND - (BAND - 1))
    col_step = lane % BAND
    keep = (row_step < bands[...]) & (col_step < bands[...])
    value = jnp.where(keep, coef[...] * scale, 0.0)
    coef[...] = jnp.where(col_step > 0, value + value, value)
    total = None
    for piece in split3(value):
        term = lax.dot_general(
            choose[...], piece, (((1,), (1,)), ((), ())), preferred_element_type=jnp.float32
        )
        total = term if total is None else total + term
    spectrum[...] = total[:, :solved]

    @pl.loop(0, strip)
    def _(h):
        ramp = dot3(coef[...], basis(row_wave[pl.ds(h, 1), :], col_wave[...]), ((1,), (1,)))
        rest = series[h] - ramp
        for c in range(items // LANES):
            piece = rest[:, c * LANES : (c + 1) * LANES]
            flat[c, pl.ds(h, coef.shape[0], stride=strip), :] = piece

    for c in range(items // LANES):
        piece = flat[c, 0 : solved * strip, :].reshape(solved, strip, LANES)
        deramped[:, :, c * LANES : (c + 1) * LANES] = piece.astype(jnp.bfloat16)

    @pl.loop(1, n_grp)
    def _(t):
        trade((grp + t) % n_grp, grp, grp).wait_send()

    @pl.loop(1, count)
    def _(t):
        dst = (me + t) % count

        @pl.when(dst < owners)
        def _():
            scatter(dst).wait_send()

        @pl.when(me < owners)
        def _():
            gather(dst).wait_send()


def choice():
    freqs = 2 * BAND - 1
    half = 2 * BAND * BAND
    table = np.zeros((freqs, freqs, 2, 2 * half), np.float32)
    for k in range(freqs):
        for m in range(freqs):
            if m >= BAND - 1:
                at, sign = k * BAND + m - (BAND - 1), -1.0
            else:
                at, sign = (freqs - 1 - k) * BAND + (BAND - 1) - m, 1.0
            table[k, m, 0, at] = 1.0
            table[k, m, 1, half + at] = sign
    return jnp.asarray(table.reshape(-1, 2 * half), jnp.bfloat16)


def on_device(stack, network, bands):
    solved = bands.shape[0]
    freqs = 2 * BAND - 1
    lanes = 4 * BAND * BAND
    n_grp, n_dev = lax.axis_size("grp"), lax.axis_size("dev")
    count = n_grp * n_dev
    share, rows_all, items = stack.shape
    ifgs, strip = share * n_grp, rows_all // n_grp
    cols_all = items * n_dev
    per = -(-solved // count)
    owners = -(-solved // per)
    tall = -(-max(solved, owners * per) // 8) * 8
    wide = -(-tall // 128) * 128
    row_pos = lax.axis_index("grp") * strip + jnp.arange(strip, dtype=jnp.int32)
    col_pos = lax.axis_index("dev") * items + jnp.arange(items, dtype=jnp.int32)
    row_wave, col_wave = wave_tables(row_pos, rows_all, col_pos, cols_all)
    bands = jnp.pad(bands, (0, tall - solved))[:, None]

    vmem = pl.BlockSpec(memory_space=pltpu.VMEM)
    f32, bf16 = jnp.float32, jnp.bfloat16
    sems = lambda n: pltpu.SemaphoreType.DMA((n,))
    deramped, fitted, spectrum = pl.pallas_call(
        functools.partial(kernel, n_grp, n_dev, solved, 1.0 / (rows_all * cols_all)),
        out_shape=(
            jax.ShapeDtypeStruct((solved, strip, items), bf16),
            jax.ShapeDtypeStruct((strip, items), f32),
            jax.ShapeDtypeStruct((2 * freqs * freqs, solved), f32),
        ),
        in_specs=[pl.BlockSpec(memory_space=pl.ANY)] + [vmem] * 5,
        out_specs=(vmem, vmem, vmem),
        scratch_shapes=[
            pltpu.VMEM((ifgs, strip, items), bf16),
            pltpu.VMEM((items // LANES, ifgs * strip, LANES), f32),
            pltpu.VMEM((wide, ifgs), bf16),
            pltpu.VMEM((tall, wide), f32),
            pltpu.VMEM((tall, ifgs), bf16),
            pltpu.VMEM((strip, tall, items), f32),
            pltpu.VMEM((tall, lanes), f32),
            pltpu.VMEM((owners, per, lanes), f32),
            pltpu.VMEM((owners, per, lanes), f32),
            pltpu.VMEM((count, per, lanes), f32),
            pltpu.VMEM((tall, lanes), f32),
            pltpu.VMEM((items // LANES, tall * strip, LANES), f32),
            sems(n_grp),
            sems(n_grp),
            pltpu.SemaphoreType.DMA,
            sems(count),
            sems(count),
            sems(count),
            sems(count),
        ],
        compiler_params=pltpu.CompilerParams(collective_id=0, has_side_effects=True),
        name="whole",
    )(stack, network.T, bands, row_wave, col_wave, choice())
    spectrum = spectrum.reshape(freqs, freqs, 2, solved).transpose(2, 3, 0, 1)
    return (deramped, fitted, spectrum)


def solution(mesh):
    return jax.shard_map(
        on_device,
        mesh=mesh,
        in_specs=(P("grp", None, "dev"), P(), P()),
        out_specs=(P(None, "grp", "dev"), P("grp", "dev"), P()),
        check_vma=False,
    )
```

```python
import functools
import math

import jax
import jax.numpy as jnp
import numpy as np
from jax import lax
from jax.experimental import pallas as pl
from jax.experimental.pallas import tpu as pltpu
from jax.sharding import PartitionSpec as P

BAND = 8
LANES = 128
MESH = pl.DeviceIdType.MESH


def waves(start, shape, step, length):
    position = start + lax.broadcasted_iota(jnp.int32, shape, 0)
    angle = (position * step % length).astype(jnp.float32) * (2.0 * math.pi / length)
    return jnp.cos(angle), jnp.sin(angle)


def split(x):
    high = x.astype(jnp.bfloat16)
    return high, (x - high.astype(jnp.float32)).astype(jnp.bfloat16)


def dot3(a, b, dims):
    (a_hi, a_lo), (b_hi, b_lo) = a, b
    dot = functools.partial(
        lax.dot_general,
        dimension_numbers=(dims, ((), ())),
        preferred_element_type=jnp.float32,
    )
    return dot(a_hi, b_hi) + (dot(a_hi, b_lo) + dot(a_lo, b_hi))


def split3(x):
    high, rest = split(x)
    low, last = split(x - high.astype(jnp.float32))
    return high, low, last


def sweep(matrix, b):
    rows, lanes = matrix.shape
    lane = lax.broadcasted_iota(jnp.int32, (8, lanes), 1)
    sub = lax.broadcasted_iota(jnp.int32, (8, lanes), 0)
    panel = matrix[pl.ds(pl.multiple_of(b * 8, 8), 8), :]
    work = pltpu.roll(panel, lanes - b * 8, axis=1)
    for r in range(8):
        inv = 1.0 / work[r : r + 1, r : r + 1]
        row = jnp.where(lane[:1] == r, 1.0, work[r : r + 1, :]) * inv
        rest = jnp.where(lane == r, 0.0, work) - work[:, r : r + 1] * row
        work = jnp.where(sub == r, row, rest)
    work = pltpu.roll(work, b * 8, axis=1)
    inside = lane // 8 == b
    unit = jnp.where(lane == sub + b * 8, 1.0, 0.0)
    zero = jnp.where(inside, 0.0, work)
    left = jnp.concatenate([jnp.where(inside, 0.0, -panel), zero, unit], axis=0)
    right = jnp.concatenate([zero, unit, jnp.where(inside, -work, work)], axis=0)
    change = lax.dot_general(
        left[:, :rows],
        right,
        (((0,), (0,)), ((), ())),
        preferred_element_type=jnp.float32,
        precision=lax.Precision.HIGHEST,
    )
    row_of = lax.broadcasted_iota(jnp.int32, (rows, lanes), 0) // 8
    lane_of = lax.broadcasted_iota(jnp.int32, (rows, lanes), 1) // 8
    matrix[...] = jnp.where((row_of == b) | (lane_of == b), 0.0, matrix[...]) + change


def inverse(solved, network, design_t, matrix, pinv):
    rows, lanes = matrix.shape
    date = lax.broadcasted_iota(jnp.int32, design_t.shape, 0) + 1
    one = lambda k: jnp.where(network[k : k + 1, :] == date, 1.0, 0.0)
    design_t[...] = (one(1) - one(0)).astype(jnp.bfloat16)
    normal = lax.dot_general(
        design_t[...],
        design_t[...],
        (((1,), (1,)), ((), ())),
        preferred_element_type=jnp.float32,
    )[:rows]
    row = lax.broadcasted_iota(jnp.int32, (rows, lanes), 0)
    lane = lax.broadcasted_iota(jnp.int32, (rows, lanes), 1)
    matrix[...] = jnp.where((row == lane) & (row >= solved), 1.0, normal)

    @pl.loop(0, rows // 8)
    def _(b):
        sweep(matrix, b)

    total = None
    for piece in split3(-matrix[...]):
        term = jnp.dot(piece, design_t[...], preferred_element_type=jnp.float32)
        total = term if total is None else total + term
    pinv[...] = total.astype(jnp.bfloat16)


def kernel(
    n_grp, n_dev, solved, scale,
    stack, network, bands, choose,
    deramped, fitted, spectrum,
    block, data, design_t, matrix, pinv, series, acc, x, y, got, coef, flat, row_wave, high, low, fit,
    send0, recv0, own, send1, recv1, send2, recv2,
):
    count = n_grp * n_dev
    grp, dev = lax.axis_index("grp"), lax.axis_index("dev")
    me = grp * n_dev + dev
    ifgs, strip, items = block.shape
    share = stack.shape[0]
    owners, per, lanes = x.shape
    tall = coef.shape[0]
    pieces, half = items // LANES, lanes // 2
    pairs = strip // 2
    rows_all, cols_all = strip * n_grp, items * n_dev

    def coords(d):
        return (d // n_dev, d % n_dev)

    barrier = pltpu.get_barrier_semaphore()

    @pl.loop(1, count)
    def _(t):
        pl.semaphore_signal(
            barrier, inc=1, device_id=coords((me + t) % count), device_id_type=MESH
        )

    pl.semaphore_wait(barrier, count - 1)

    def part(ref, c, start, rows, strips=None):
        cols = pl.ds(c * LANES, LANES)
        if strips is None:
            return ref.at[pl.ds(start, rows), :, cols]
        return ref.at[:, pl.ds(pl.multiple_of(strips * strip, strip), strip), cols]

    def trade(c, to, slot, place):
        return pltpu.make_async_remote_copy(
            src_ref=part(stack, c, 0, share, to),
            dst_ref=part(block, c, place * share, share),
            send_sem=send0.at[c, to],
            recv_sem=recv0.at[c, slot],
            device_id=(to, dev),
            device_id_type=MESH,
        )

    def local(c):
        return pltpu.make_async_copy(
            part(stack, c, 0, share, grp), part(block, c, grp * share, share), own.at[c]
        )

    for c in range(pieces):

        @pl.loop(1, n_grp)
        def _(t):
            trade(c, (grp + t) % n_grp, grp, grp).start()

        local(c).start()

    inverse(solved, network, design_t, matrix, pinv)

    step = lax.broadcasted_iota(jnp.int32, (strip, half), 1) // BAND - (BAND - 1)
    row_cos, row_sin = waves(grp * strip, step.shape, step, rows_all)
    row_wave[:, :half] = row_cos
    row_wave[:, half:] = row_sin
    for c in range(pieces):
        step = lax.broadcasted_iota(jnp.int32, (LANES, half), 1) % BAND
        col_cos, col_sin = waves(dev * items + c * LANES, step.shape, step, cols_all)

        @pl.loop(0, pairs)
        def _(q):
            for e in range(2):
                row = row_wave[pl.ds(q * 2 + e, 1), :]
                row_cos, row_sin = row[:, :half], row[:, half:]
                cos = split(row_cos * col_cos - row_sin * col_sin)
                sin = split(row_sin * col_cos + row_cos * col_sin)
                at = pl.ds(e * LANES, LANES)
                for ref, i in ((high, 0), (low, 1)):
                    ref[c * pairs + q, at, :half] = cos[i]
                    ref[c * pairs + q, at, half:] = sin[i]

    acc[...] = jnp.zeros_like(acc)

    def widen(c, src):
        piece = block[pl.ds(src * share, share), :, c * LANES : (c + 1) * LANES]
        start = pl.multiple_of(src * share * strip, strip)
        piece = piece.astype(jnp.float32).reshape(share * strip, LANES)
        data[c, pl.ds(start, share * strip), :] = piece

    for c in range(pieces):
        local(c).wait()
        widen(c, grp)

        @pl.loop(1, n_grp)
        def _(t):
            src = (grp + n_grp - t) % n_grp
            trade(c, src, src, src).wait_recv()
            widen(c, src)

        @pl.loop(0, pairs)
        def _(q):
            g = c * pairs + q
            phase = jnp.concatenate(
                [data[c, pl.ds(q * 2 + e, ifgs, stride=strip), :] for e in range(2)], axis=1
            )
            out = jnp.dot(
                pinv[...], phase.astype(jnp.bfloat16), preferred_element_type=jnp.float32
            )
            series[g] = out
            model = lax.dot_general(
                design_t[0:tall, :],
                out.astype(jnp.bfloat16),
                (((0,), (0,)), ((), ())),
                preferred_element_type=jnp.float32,
            )
            resid = phase - model
            mean = jnp.sum(resid * resid, axis=0, keepdims=True) * (1.0 / ifgs)
            value = jnp.sqrt(mean + 1e-06)
            for e in range(2):
                fit[c, pl.ds(q * 2 + e, 1), :] = value[:, e * LANES : (e + 1) * LANES]
            acc[...] += dot3(split(out), (high[g], low[g]), ((1,), (0,)))

        fitted[:, c * LANES : (c + 1) * LANES] = fit[c]

    for j in range(owners):
        x[j] = acc[j * per : (j + 1) * per, :]

    def scatter(dst):
        return pltpu.make_async_remote_copy(
            src_ref=x.at[dst],
            dst_ref=got.at[me],
            send_sem=send1.at[dst],
            recv_sem=recv1.at[me],
            device_id=coords(dst),
            device_id_type=MESH,
        )

    def gather(dst):
        return pltpu.make_async_remote_copy(
            src_ref=y.at[me],
            dst_ref=y.at[me],
            send_sem=send2.at[dst],
            recv_sem=recv2.at[me],
            device_id=coords(dst),
            device_id_type=MESH,
        )

    @pl.loop(1, count)
    def _(t):
        dst = (me + t) % count

        @pl.when(dst < owners)
        def _():
            scatter(dst).start()

    @pl.when(me < owners)
    def _():
        y[me] = x[me]

        @pl.loop(1, count)
        def _(t):
            src = (me + count - t) % count
            pltpu.make_async_remote_copy(
                src_ref=x.at[0],
                dst_ref=got.at[src],
                send_sem=send1.at[src],
                recv_sem=recv1.at[src],
                device_id=coords(src),
                device_id_type=MESH,
            ).wait_recv()
            y[me] += got[src]

        @pl.loop(1, count)
        def _(t):
            gather((me + t) % count).start()

    @pl.loop(1, count)
    def _(t):
        src = (me + count - t) % count

        @pl.when(src < owners)
        def _():
            pltpu.make_async_remote_copy(
                src_ref=y.at[0],
                dst_ref=y.at[src],
                send_sem=send2.at[src],
                recv_sem=recv2.at[src],
                device_id=coords(src),
                device_id_type=MESH,
            ).wait_recv()

    coef[...] = jnp.zeros_like(coef)
    for j in range(owners):
        coef[j * per : (j + 1) * per, :] = y[j]

    lane = lax.broadcasted_iota(jnp.int32, coef.shape, 1) % (2 * BAND * BAND)
    row_step = jnp.abs(lane // BAND - (BAND - 1))
    col_step = lane % BAND
    date = lax.broadcasted_iota(jnp.int32, (tall, solved), 0)
    same = date == lax.broadcasted_iota(jnp.int32, (tall, solved), 1)
    band = jnp.where(same, bands[...].astype(jnp.float32), 0.0)
    band = jnp.sum(band, axis=1, keepdims=True)
    keep = jnp.maximum(row_step, col_step).astype(jnp.float32) < band
    value = jnp.where(keep, coef[...] * scale, 0.0)
    weighted = split(jnp.where(col_step > 0, value + value, value))
    parts = split3(value)
    for i in range(2):
        total = None
        for piece in parts:
            term = lax.dot_general(
                choose[i], piece, (((1,), (1,)), ((), ())), preferred_element_type=jnp.float32
            )
            total = term if total is None else total + term
        spectrum[i] = total[:, :solved]

    for c in range(pieces):

        @pl.loop(0, pairs)
        def _(q):
            g = c * pairs + q
            rest = series[g] - dot3(weighted, (high[g], low[g]), ((1,), (1,)))
            for e in range(2):
                piece = rest[:, e * LANES : (e + 1) * LANES]
                flat[c, pl.ds(q * 2 + e, tall, stride=strip), :] = piece

        piece = flat[c, 0 : solved * strip, :].reshape(solved, strip, LANES)
        deramped[:, :, c * LANES : (c + 1) * LANES] = piece.astype(jnp.bfloat16)

    for c in range(pieces):

        @pl.loop(1, n_grp)
        def _(t):
            trade(c, (grp + t) % n_grp, grp, grp).wait_send()

    @pl.loop(1, count)
    def _(t):
        dst = (me + t) % count

        @pl.when(dst < owners)
        def _():
            scatter(dst).wait_send()

        @pl.when(me < owners)
        def _():
            gather(dst).wait_send()


def choice():
    freqs = 2 * BAND - 1
    half = 2 * BAND * BAND
    table = np.zeros((2, freqs, freqs, 2 * half), np.float32)
    for k in range(freqs):
        for m in range(freqs):
            if m >= BAND - 1:
                at, sign = k * BAND + m - (BAND - 1), -1.0
            else:
                at, sign = (freqs - 1 - k) * BAND + (BAND - 1) - m, 1.0
            table[0, k, m, at] = 1.0
            table[1, k, m, half + at] = sign
    return jnp.asarray(table.reshape(2, -1, 2 * half), jnp.bfloat16)


def on_device(stack, network, bands):
    solved = bands.shape[0]
    freqs = 2 * BAND - 1
    lanes = 4 * BAND * BAND
    n_grp, n_dev = lax.axis_size("grp"), lax.axis_size("dev")
    count = n_grp * n_dev
    share, rows_all, items = stack.shape
    ifgs, strip = share * n_grp, rows_all // n_grp
    cols_all = items * n_dev
    per = -(-solved // count)
    owners = -(-solved // per)
    tall = -(-max(solved, owners * per) // 8) * 8
    wide = -(-tall // 128) * 128
    vmem = pl.BlockSpec(memory_space=pltpu.VMEM)
    f32, bf16 = jnp.float32, jnp.bfloat16
    sems = lambda *n: pltpu.SemaphoreType.DMA(n)
    pieces = items // LANES
    groups = pieces * strip // 2
    deramped, fitted, spectrum = pl.pallas_call(
        functools.partial(kernel, n_grp, n_dev, solved, 1.0 / (rows_all * cols_all)),
        out_shape=(
            jax.ShapeDtypeStruct((solved, strip, items), bf16),
            jax.ShapeDtypeStruct((strip, items), f32),
            jax.ShapeDtypeStruct((2, freqs * freqs, solved), f32),
        ),
        in_specs=[pl.BlockSpec(memory_space=pl.ANY)] + [vmem] * 3,
        out_specs=(vmem, vmem, vmem),
        scratch_shapes=[
            pltpu.VMEM((ifgs, strip, items), bf16),
            pltpu.VMEM((items // LANES, ifgs * strip, LANES), f32),
            pltpu.VMEM((wide, ifgs), bf16),
            pltpu.VMEM((tall, wide), f32),
            pltpu.VMEM((tall, ifgs), bf16),
            pltpu.VMEM((groups, tall, 2 * LANES), f32),
            pltpu.VMEM((tall, lanes), f32),
            pltpu.VMEM((owners, per, lanes), f32),
            pltpu.VMEM((owners, per, lanes), f32),
            pltpu.VMEM((count, per, lanes), f32),
            pltpu.VMEM((tall, lanes), f32),
            pltpu.VMEM((pieces, tall * strip, LANES), f32),
            pltpu.VMEM((strip, lanes), f32),
            pltpu.VMEM((groups, 2 * LANES, lanes), bf16),
            pltpu.VMEM((groups, 2 * LANES, lanes), bf16),
            pltpu.VMEM((pieces, strip, LANES), f32),
            sems(pieces, n_grp),
            sems(pieces, n_grp),
            sems(pieces),
            sems(count),
            sems(count),
            sems(count),
            sems(count),
        ],
        compiler_params=pltpu.CompilerParams(collective_id=0, has_side_effects=True),
        name="whole",
    )(stack, network.T, bands[None, :], choice())
    spectrum = spectrum.transpose(1, 0, 2).reshape(freqs, freqs, 2, solved)
    spectrum = spectrum.transpose(2, 3, 0, 1)
    return (deramped, fitted, spectrum)


def solution(mesh):
    return jax.shard_map(
        on_device,
        mesh=mesh,
        in_specs=(P("grp", None, "dev"), P(), P()),
        out_specs=(P(None, "grp", "dev"), P("grp", "dev"), P()),
        check_vma=False,
    )
```

```python
import functools
import math

import jax
import jax.numpy as jnp
import numpy as np
from jax import lax
from jax.experimental import pallas as pl
from jax.experimental.pallas import tpu as pltpu
from jax.sharding import PartitionSpec as P

BAND = 8
LANES = 128
MESH = pl.DeviceIdType.MESH


def waves(start, shape, step, length):
    position = start + lax.broadcasted_iota(jnp.int32, shape, 0)
    angle = (position * step % length).astype(jnp.float32) * (2.0 * math.pi / length)
    return jnp.cos(angle), jnp.sin(angle)


def split(x):
    high = x.astype(jnp.bfloat16)
    return high, (x - high.astype(jnp.float32)).astype(jnp.bfloat16)


def dot3(a, b, dims):
    (a_hi, a_lo), (b_hi, b_lo) = a, b
    dot = functools.partial(
        lax.dot_general,
        dimension_numbers=(dims, ((), ())),
        preferred_element_type=jnp.float32,
    )
    return dot(a_hi, b_hi) + (dot(a_hi, b_lo) + dot(a_lo, b_hi))


def split3(x):
    high, rest = split(x)
    low, last = split(x - high.astype(jnp.float32))
    return high, low, last


def sweep(matrix, b):
    rows, lanes = matrix.shape
    lane = lax.broadcasted_iota(jnp.int32, (8, lanes), 1)
    sub = lax.broadcasted_iota(jnp.int32, (8, lanes), 0)
    panel = matrix[pl.ds(pl.multiple_of(b * 8, 8), 8), :]
    work = pltpu.roll(panel, lanes - b * 8, axis=1)
    for r in range(8):
        inv = 1.0 / work[r : r + 1, r : r + 1]
        row = jnp.where(lane[:1] == r, 1.0, work[r : r + 1, :]) * inv
        rest = jnp.where(lane == r, 0.0, work) - work[:, r : r + 1] * row
        work = jnp.where(sub == r, row, rest)
    work = pltpu.roll(work, b * 8, axis=1)
    inside = lane // 8 == b
    unit = jnp.where(lane == sub + b * 8, 1.0, 0.0)
    zero = jnp.where(inside, 0.0, work)
    left = jnp.concatenate([jnp.where(inside, 0.0, -panel), zero, unit], axis=0)
    right = jnp.concatenate([zero, unit, jnp.where(inside, -work, work)], axis=0)
    change = lax.dot_general(
        left[:, :rows],
        right,
        (((0,), (0,)), ((), ())),
        preferred_element_type=jnp.float32,
        precision=lax.Precision.HIGHEST,
    )
    row_of = lax.broadcasted_iota(jnp.int32, (rows, lanes), 0) // 8
    lane_of = lax.broadcasted_iota(jnp.int32, (rows, lanes), 1) // 8
    matrix[...] = jnp.where((row_of == b) | (lane_of == b), 0.0, matrix[...]) + change


def inverse(solved, network, design_t, matrix, pinv):
    rows, lanes = matrix.shape
    date = lax.broadcasted_iota(jnp.int32, design_t.shape, 0) + 1
    one = lambda k: jnp.where(network[k : k + 1, :] == date, 1.0, 0.0)
    design_t[...] = (one(1) - one(0)).astype(jnp.bfloat16)
    normal = lax.dot_general(
        design_t[...],
        design_t[...],
        (((1,), (1,)), ((), ())),
        preferred_element_type=jnp.float32,
    )[:rows]
    row = lax.broadcasted_iota(jnp.int32, (rows, lanes), 0)
    lane = lax.broadcasted_iota(jnp.int32, (rows, lanes), 1)
    matrix[...] = jnp.where((row == lane) & (row >= solved), 1.0, normal)

    @pl.loop(0, rows // 8)
    def _(b):
        sweep(matrix, b)

    total = None
    for piece in split3(-matrix[...]):
        term = jnp.dot(piece, design_t[...], preferred_element_type=jnp.float32)
        total = term if total is None else total + term
    pinv[...] = total.astype(jnp.bfloat16)


def kernel(
    n_grp, n_dev, solved, scale,
    stack, network, bands, choose,
    deramped, fitted, spectrum,
    block, data, design_t, matrix, pinv, series, acc, x, y, got, coef, flat, row_wave, high, low, fit,
    send0, recv0, own, send1, recv1, send2, recv2,
):
    count = n_grp * n_dev
    grp, dev = lax.axis_index("grp"), lax.axis_index("dev")
    me = grp * n_dev + dev
    ifgs, strip, items = block.shape
    share = stack.shape[0]
    owners, per, lanes = x.shape
    tall = coef.shape[0]
    pieces, half = items // LANES, lanes // 2
    pairs = strip // 2
    rows_all, cols_all = strip * n_grp, items * n_dev

    def coords(d):
        return (lax.div(d, n_dev), lax.rem(d, n_dev))

    barrier = pltpu.get_barrier_semaphore()

    @pl.loop(1, count)
    def _(t):
        pl.semaphore_signal(
            barrier, inc=1, device_id=coords(lax.rem(me + t, count)), device_id_type=MESH
        )

    pl.semaphore_wait(barrier, count - 1)

    def part(ref, c, start, rows, strips=None):
        cols = pl.ds(c * LANES, LANES)
        if strips is None:
            return ref.at[pl.ds(start, rows), :, cols]
        return ref.at[:, pl.ds(pl.multiple_of(strips * strip, strip), strip), cols]

    def trade(c, to, slot, place):
        return pltpu.make_async_remote_copy(
            src_ref=part(stack, c, 0, share, to),
            dst_ref=part(block, c, place * share, share),
            send_sem=send0.at[c, to],
            recv_sem=recv0.at[c, slot],
            device_id=(to, dev),
            device_id_type=MESH,
        )

    def local(c):
        return pltpu.make_async_copy(
            part(stack, c, 0, share, grp), part(block, c, grp * share, share), own.at[c]
        )

    for c in range(pieces):

        @pl.loop(1, n_grp)
        def _(t):
            trade(c, (grp + t) % n_grp, grp, grp).start()

        local(c).start()

    inverse(solved, network, design_t, matrix, pinv)

    step = lax.broadcasted_iota(jnp.int32, (strip, half), 1) // BAND - (BAND - 1)
    row_cos, row_sin = waves(grp * strip, step.shape, step, rows_all)
    row_wave[:, :half] = row_cos
    row_wave[:, half:] = row_sin
    for c in range(pieces):
        step = lax.broadcasted_iota(jnp.int32, (LANES, half), 1) % BAND
        col_cos, col_sin = waves(dev * items + c * LANES, step.shape, step, cols_all)

        @pl.loop(0, pairs)
        def _(q):
            for e in range(2):
                row = row_wave[pl.ds(q * 2 + e, 1), :]
                row_cos, row_sin = row[:, :half], row[:, half:]
                cos = split(row_cos * col_cos - row_sin * col_sin)
                sin = split(row_sin * col_cos + row_cos * col_sin)
                at = pl.ds(e * LANES, LANES)
                for ref, i in ((high, 0), (low, 1)):
                    ref[c * pairs + q, at, :half] = cos[i]
                    ref[c * pairs + q, at, half:] = sin[i]

    acc[...] = jnp.zeros_like(acc)

    def widen(c, src):
        piece = block[pl.ds(src * share, share), :, c * LANES : (c + 1) * LANES]
        start = pl.multiple_of(src * share * strip, strip)
        piece = piece.astype(jnp.float32).reshape(share * strip, LANES)
        data[c, pl.ds(start, share * strip), :] = piece

    for c in range(pieces):
        local(c).wait()
        widen(c, grp)

        @pl.loop(1, n_grp)
        def _(t):
            src = (grp + n_grp - t) % n_grp
            trade(c, src, src, src).wait_recv()
            widen(c, src)

        @pl.loop(0, pairs)
        def _(q):
            g = c * pairs + q
            phase = jnp.concatenate(
                [data[c, pl.ds(q * 2 + e, ifgs, stride=strip), :] for e in range(2)], axis=1
            )
            out = jnp.dot(
                pinv[...], phase.astype(jnp.bfloat16), preferred_element_type=jnp.float32
            )
            series[g] = out
            model = lax.dot_general(
                design_t[0:tall, :],
                out.astype(jnp.bfloat16),
                (((0,), (0,)), ((), ())),
                preferred_element_type=jnp.float32,
            )
            resid = phase - model
            mean = jnp.sum(resid * resid, axis=0, keepdims=True) * (1.0 / ifgs)
            value = jnp.sqrt(mean + 1e-06)
            for e in range(2):
                fit[c, pl.ds(q * 2 + e, 1), :] = value[:, e * LANES : (e + 1) * LANES]
            acc[...] += dot3(split(out), (high[g], low[g]), ((1,), (0,)))

        fitted[:, c * LANES : (c + 1) * LANES] = fit[c]

    for j in range(owners):
        x[j] = acc[j * per : (j + 1) * per, :]

    def scatter(dst):
        return pltpu.make_async_remote_copy(
            src_ref=x.at[dst],
            dst_ref=got.at[me],
            send_sem=send1.at[dst],
            recv_sem=recv1.at[me],
            device_id=coords(dst),
            device_id_type=MESH,
        )

    def gather(dst):
        return pltpu.make_async_remote_copy(
            src_ref=y.at[me],
            dst_ref=y.at[me],
            send_sem=send2.at[dst],
            recv_sem=recv2.at[me],
            device_id=coords(dst),
            device_id_type=MESH,
        )

    @pl.loop(1, count)
    def _(t):
        dst = lax.rem(me + t, count)

        @pl.when(dst < owners)
        def _():
            scatter(dst).start()

    @pl.when(me < owners)
    def _():
        got[me] = x[me]

        @pl.loop(0, count, unroll=4)
        def _(src):
            @pl.when(src != me)
            def _():
                pltpu.make_async_remote_copy(
                    src_ref=x.at[0],
                    dst_ref=got.at[src],
                    send_sem=send1.at[src],
                    recv_sem=recv1.at[src],
                    device_id=(grp, dev),
                    device_id_type=MESH,
                ).wait_recv()

        y[me] = jnp.sum(got[...], axis=0)

        @pl.loop(1, count)
        def _(t):
            gather(lax.rem(me + t, count)).start()

    @pl.loop(0, owners)
    def _(src):
        @pl.when(src != me)
        def _():
            pltpu.make_async_remote_copy(
                src_ref=y.at[0],
                dst_ref=y.at[src],
                send_sem=send2.at[src],
                recv_sem=recv2.at[src],
                device_id=(grp, dev),
                device_id_type=MESH,
            ).wait_recv()

    coef[...] = jnp.zeros_like(coef)
    for j in range(owners):
        coef[j * per : (j + 1) * per, :] = y[j]

    lane = lax.broadcasted_iota(jnp.int32, coef.shape, 1) % (2 * BAND * BAND)
    row_step = jnp.abs(lane // BAND - (BAND - 1))
    col_step = lane % BAND
    date = lax.broadcasted_iota(jnp.int32, (tall, solved), 0)
    same = date == lax.broadcasted_iota(jnp.int32, (tall, solved), 1)
    band = jnp.where(same, bands[...].astype(jnp.float32), 0.0)
    band = jnp.sum(band, axis=1, keepdims=True)
    keep = jnp.maximum(row_step, col_step).astype(jnp.float32) < band
    value = jnp.where(keep, coef[...] * scale, 0.0)
    weighted = split(jnp.where(col_step > 0, value + value, value))
    parts = split3(value)
    for i in range(2):
        total = None
        for piece in parts:
            term = lax.dot_general(
                choose[i], piece, (((1,), (1,)), ((), ())), preferred_element_type=jnp.float32
            )
            total = term if total is None else total + term
        spectrum[i] = total[:, :solved]

    for c in range(pieces):

        @pl.loop(0, pairs)
        def _(q):
            g = c * pairs + q
            rest = series[g] - dot3(weighted, (high[g], low[g]), ((1,), (1,)))
            for e in range(2):
                piece = rest[:, e * LANES : (e + 1) * LANES]
                flat[c, pl.ds(q * 2 + e, tall, stride=strip), :] = piece

        piece = flat[c, 0 : solved * strip, :].reshape(solved, strip, LANES)
        deramped[:, :, c * LANES : (c + 1) * LANES] = piece.astype(jnp.bfloat16)

    for c in range(pieces):

        @pl.loop(1, n_grp)
        def _(t):
            trade(c, (grp + t) % n_grp, grp, grp).wait_send()

    @pl.loop(1, count)
    def _(t):
        dst = lax.rem(me + t, count)

        @pl.when(dst < owners)
        def _():
            scatter(dst).wait_send()

        @pl.when(me < owners)
        def _():
            gather(dst).wait_send()


def choice():
    freqs = 2 * BAND - 1
    half = 2 * BAND * BAND
    table = np.zeros((2, freqs, freqs, 2 * half), np.float32)
    for k in range(freqs):
        for m in range(freqs):
            if m >= BAND - 1:
                at, sign = k * BAND + m - (BAND - 1), -1.0
            else:
                at, sign = (freqs - 1 - k) * BAND + (BAND - 1) - m, 1.0
            table[0, k, m, at] = 1.0
            table[1, k, m, half + at] = sign
    return jnp.asarray(table.reshape(2, -1, 2 * half), jnp.bfloat16)


def on_device(stack, network, bands):
    solved = bands.shape[0]
    freqs = 2 * BAND - 1
    lanes = 4 * BAND * BAND
    n_grp, n_dev = lax.axis_size("grp"), lax.axis_size("dev")
    count = n_grp * n_dev
    share, rows_all, items = stack.shape
    ifgs, strip = share * n_grp, rows_all // n_grp
    cols_all = items * n_dev
    per = -(-solved // count)
    owners = -(-solved // per)
    tall = -(-max(solved, owners * per) // 8) * 8
    wide = -(-tall // 128) * 128
    vmem = pl.BlockSpec(memory_space=pltpu.VMEM)
    f32, bf16 = jnp.float32, jnp.bfloat16
    sems = lambda *n: pltpu.SemaphoreType.DMA(n)
    pieces = items // LANES
    groups = pieces * strip // 2
    deramped, fitted, spectrum = pl.pallas_call(
        functools.partial(kernel, n_grp, n_dev, solved, 1.0 / (rows_all * cols_all)),
        out_shape=(
            jax.ShapeDtypeStruct((solved, strip, items), bf16),
            jax.ShapeDtypeStruct((strip, items), f32),
            jax.ShapeDtypeStruct((2, freqs * freqs, solved), f32),
        ),
        in_specs=[pl.BlockSpec(memory_space=pl.ANY)] + [vmem] * 3,
        out_specs=(vmem, vmem, vmem),
        scratch_shapes=[
            pltpu.VMEM((ifgs, strip, items), bf16),
            pltpu.VMEM((items // LANES, ifgs * strip, LANES), f32),
            pltpu.VMEM((wide, ifgs), bf16),
            pltpu.VMEM((tall, wide), f32),
            pltpu.VMEM((tall, ifgs), bf16),
            pltpu.VMEM((groups, tall, 2 * LANES), f32),
            pltpu.VMEM((tall, lanes), f32),
            pltpu.VMEM((owners, per, lanes), f32),
            pltpu.VMEM((owners, per, lanes), f32),
            pltpu.VMEM((count, per, lanes), f32),
            pltpu.VMEM((tall, lanes), f32),
            pltpu.VMEM((pieces, tall * strip, LANES), f32),
            pltpu.VMEM((strip, lanes), f32),
            pltpu.VMEM((groups, 2 * LANES, lanes), bf16),
            pltpu.VMEM((groups, 2 * LANES, lanes), bf16),
            pltpu.VMEM((pieces, strip, LANES), f32),
            sems(pieces, n_grp),
            sems(pieces, n_grp),
            sems(pieces),
            sems(count),
            sems(count),
            sems(count),
            sems(count),
        ],
        compiler_params=pltpu.CompilerParams(collective_id=0, has_side_effects=True),
        name="whole",
    )(stack, network.T, bands[None, :], choice())
    spectrum = spectrum.transpose(1, 0, 2).reshape(freqs, freqs, 2, solved)
    spectrum = spectrum.transpose(2, 3, 0, 1)
    return (deramped, fitted, spectrum)


def solution(mesh):
    return jax.shard_map(
        on_device,
        mesh=mesh,
        in_specs=(P("grp", None, "dev"), P(), P()),
        out_specs=(P(None, "grp", "dev"), P("grp", "dev"), P()),
        check_vma=False,
    )
```
